256 devices in a mesh: group: 64 (over z, y_hi, x), replica: 4 (over y_lo, core).
Axes of the slice: x: 4, y: 4 (y_hi: 2, y_lo: 2; y = y_hi * 2 + y_lo), z: 8, core: 2. Of those that a mesh axis runs over, the one named last changes fastest.
Arguments:
- grad: bfloat16 [32768, 8192], P('group', 'replica'), may hold values from -45 to 45, as said below
- prev_left: bfloat16 [64, 512, 512], P('group', 'replica'), may hold values from -1 to 1.5
- prev_right: bfloat16 [16, 512, 512], P('replica', 'group'), may hold values from -1 to 1.5
- exp_left: int32 [64], P('group'), may hold values from -2 to 2
- exp_right: int32 [16], P('replica'), may hold values from -2 to 2
- strip_owner: int32 [64], replicated, may hold values from 0 to 63, each once
Outputs:
- precond: bfloat16 [32768, 8192], P('group', 'replica')
- root_left: bfloat16 [64, 512, 512], P('group', 'replica')
- root_right: bfloat16 [16, 64, 8, 512], P('replica', 'group')
The draws below stay inside these ranges and needn't reach their ends.
Inputs may be any that keep to these rules, and one draw needn't show every extreme that they name: `grad`: entries have row and column scales of different sizes. `strip_owner`: each of 0 to 63 appears once.
All inputs are finite; a program needn't handle non-finite values.
Results may differ from the reference program's by a relative error of at most 0.0083.
Values may be sent and summed in bfloat16 or wider, within the bound.
A program may use at most 64 MiB of HBM per device.

```python
import math
import jax
import jax.numpy as jnp
from jax import lax

BLOCK = 512
ROW_BLOCKS = 64
COL_BLOCKS = 16
ROWS = 32768
COLS = 8192
RSTRIP = 8
N_GROUP = 64


def draw_grad(key, part):
    keys = jax.random.split(key, 3)
    row_scale = jnp.exp(jax.random.uniform(keys[0], (ROWS, 1), jnp.float32, math.log(0.3), math.log(3.0)))
    column_scale = jnp.exp(jax.random.uniform(keys[1], (1, COLS), jnp.float32, math.log(0.3), math.log(3.0)))
    entries = jax.random.normal(keys[2], (ROWS, COLS), jnp.float32)
    entries = jnp.clip(entries, -5.0, 5.0)
    return (entries * row_scale * column_scale).astype(jnp.bfloat16)


def make_roots(key, count):
    keys = jax.random.split(key, 2)
    diagonal = jnp.exp(jax.random.uniform(keys[0], (count, BLOCK), jnp.float32, math.log(0.8), math.log(1.25)))
    spread = 0.25 / math.sqrt(BLOCK)
    offdiag = jnp.clip(jax.random.normal(keys[1], (count, BLOCK, BLOCK), jnp.float32), -5.0, 5.0) * spread
    identity = jnp.eye(BLOCK, dtype=jnp.float32)
    return (offdiag + identity[None, :, :] * diagonal[:, :, None]).astype(jnp.bfloat16)


def draw_prev_left(key, part):
    return make_roots(jax.random.fold_in(key, 11), ROW_BLOCKS)


def draw_prev_right(key, part):
    return make_roots(jax.random.fold_in(key, 23), COL_BLOCKS)


def plant(array, stream_key, least, top_value):
    longest = array.shape.index(max(array.shape))
    spots = []
    for shift in (0, 1):
        where = [jax.random.randint(jax.random.fold_in(stream_key, axis), (), 0, length) for axis, length in enumerate(array.shape)]
        where[longest] = (where[longest] + shift) % array.shape[longest]
        spots.append(tuple(where))
    return array.at[spots[0]].set(least).at[spots[1]].set(top_value)


def setup_inputs(seed: int = 0) -> dict:
    key_list = jax.random.split(jax.random.key(seed), 7)
    grad = draw_grad(jax.random.fold_in(key_list[6], 71), 0)
    prev_left = draw_prev_left(jax.random.fold_in(key_list[6], 71), 0)
    prev_right = draw_prev_right(jax.random.fold_in(key_list[6], 71), 0)
    exp_left = plant(jax.random.randint(key_list[3], (ROW_BLOCKS,), -2, 3), jax.random.fold_in(key_list[3], 1), -2, 2).astype(jnp.int32)
    exp_right = plant(jax.random.randint(key_list[4], (COL_BLOCKS,), -2, 3), jax.random.fold_in(key_list[4], 1), -2, 2).astype(jnp.int32)
    strip_owner = jax.random.permutation(key_list[5], ROW_BLOCKS).astype(jnp.int32)
    return dict(grad=grad, prev_left=prev_left, prev_right=prev_right, exp_left=exp_left, exp_right=exp_right, strip_owner=strip_owner)


EPSILON = 1e-6


def pow_two(exponent):
    result = jnp.zeros(exponent.shape, jnp.float32)
    for power in range(-4, 5):
        result = result + jnp.where(exponent == power, jnp.float32(2.0 ** power), jnp.float32(0.0))
    return result


def newton_step(gram, gram_scale, start_root):
    product = gram / gram_scale
    for repeat in range(5):
        product = jnp.dot(product, start_root, precision=lax.Precision.HIGHEST)
    return (5.0 * start_root - product) / 4.0


def reference(grad, prev_left, prev_right, exp_left, exp_right, strip_owner):
    blocks = grad.reshape(N_GROUP, BLOCK, COL_BLOCKS, BLOCK).transpose(0, 2, 1, 3)
    squares = jnp.sum(jnp.square(blocks.astype(jnp.float32)), axis=(2, 3))
    left_scale = jnp.sum(squares, axis=1) / BLOCK + EPSILON
    right_scale = jnp.sum(squares, axis=0) / BLOCK + EPSILON

    def left_gram_of(row_blocks):
        running = jnp.zeros((BLOCK, BLOCK), jnp.float32)
        for column in range(COL_BLOCKS):
            piece = row_blocks[column]
            running = running + jnp.dot(piece, piece.T, preferred_element_type=jnp.float32)
        return running

    left_gram = lax.map(left_gram_of, blocks)

    def add_right(carry, row_blocks):
        terms = []
        for column in range(COL_BLOCKS):
            piece = row_blocks[column]
            terms.append(jnp.dot(piece.T, piece, preferred_element_type=jnp.float32))
        return carry + jnp.stack(terms), None

    right_gram, unused = lax.scan(add_right, jnp.zeros((COL_BLOCKS, BLOCK, BLOCK), jnp.float32), blocks)

    def left_one(packed):
        gram, gram_scale, start_root = packed
        return newton_step(gram, gram_scale, start_root.astype(jnp.float32))

    left_new = lax.map(left_one, (left_gram, left_scale, prev_left))
    root_left = (left_new * pow_two(-exp_left)[:, None, None]).astype(jnp.bfloat16)
    right_codes = []
    for column in range(COL_BLOCKS):
        right_new = newton_step(right_gram[column], right_scale[column], prev_right[column].astype(jnp.float32))
        right_codes.append((right_new * pow_two(-exp_right[column])).astype(jnp.bfloat16))
    code_right = jnp.stack(right_codes)
    root_right = code_right.reshape(COL_BLOCKS, N_GROUP, RSTRIP, BLOCK)[:, strip_owner]
    dec_left = (root_left.astype(jnp.float32) * pow_two(exp_left)[:, None, None]).astype(jnp.bfloat16)
    dec_right = (code_right.astype(jnp.float32) * pow_two(exp_right)[:, None, None]).astype(jnp.bfloat16)

    def precondition(packed):
        row_blocks, left_root = packed
        outputs = []
        for column in range(COL_BLOCKS):
            middle = jnp.dot(row_blocks[column], dec_right[column], preferred_element_type=jnp.float32).astype(jnp.bfloat16)
            outputs.append(jnp.dot(left_root, middle, preferred_element_type=jnp.float32).astype(jnp.bfloat16))
        return jnp.stack(outputs)

    result_blocks = lax.map(precondition, (blocks, dec_left))
    precond = result_blocks.transpose(0, 2, 1, 3).reshape(N_GROUP * BLOCK, COL_BLOCKS * BLOCK)
    return precond, root_left, root_right
```

```python
import functools

import jax
import jax.numpy as jnp
from jax import lax
from jax.experimental import pallas as pl
from jax.experimental.pallas import tpu as pltpu
from jax.sharding import Mesh
from jax.sharding import PartitionSpec as P

AXES = ("z", "yh", "x", "yl", "c")
GROUP = ("z", "yh", "x")
REPLICA = ("yl", "c")
MESH_ID = pl.DeviceIdType.MESH
F32 = jnp.float32
BF16 = jnp.bfloat16

EPSILON = 1e-06
B = 512
CUT = 384
ROUNDS = 4
PLANE = ((0, 1), (1, 0), (0, 3), (0, 2), (1, 1), (1, 3), (1, 2))
DEPTH = (1, 7, 2, 6, 3, 5, 4)


def pow_two(exponent):
    result = jnp.float32(0.0)
    for power in range(-4, 5):
        result = result + jnp.where(exponent == power, jnp.float32(2.0**power), jnp.float32(0.0))
    return result


def five_products(rows, root):
    count = rows.shape[0]
    for repeat in range(5):
        high = rows.astype(BF16)
        low = (rows - high.astype(F32)).astype(BF16)
        both = jnp.dot(jnp.concatenate([high, low], axis=0), root, preferred_element_type=F32)
        rows = both[:count] + both[count:]
    return rows


def exchange_kernel(
    exp_left, exp_right, owner_of, grad, prev_left, prev_right,
    middle, left_all, left_own, right_own,
    gram, plane_in, depth_in, plane_sum, depth_sum, strip_z, strip_p,
    norm_own, norm_mid, norm_p, norm_z,
    xz, xp, root, code,
    lgram, lin1, lsend, lin2, lroot, lcode, lnorm, lnorm_in,
    sem_plane, sem_depth, sem_sz, sem_sp, sem_n1, sem_n2, sem_xz, sem_xp,
    sem_cz, sem_cp, sem_fp, sem_fz, sem_l,
):
    z, yh, x = lax.axis_index("z"), lax.axis_index("yh"), lax.axis_index("x")
    yl, c = lax.axis_index("yl"), lax.axis_index("c")
    p = yh * 4 + x
    me_r = p // 2

    def plane_peer(step):
        return ((yh + step[0]) % 2, (x + step[1]) % 4)

    def plane_id(step):
        a, b = plane_peer(step)
        return (z, a, b, yl, c)

    def depth_id(step):
        return ((z + step) % 8, yh, x, yl, c)

    core_id = (z, yh, x, yl, 1 - c)
    side_id = (z, yh, x, 1 - yl, c)

    def send(src, dst, sems, device):
        copy = pltpu.make_async_remote_copy(
            src_ref=src, dst_ref=dst, send_sem=sems[0], recv_sem=sems[1],
            device_id=device, device_id_type=MESH_ID,
        )
        copy.start()
        return copy

    def two(sem, *index):
        return sem.at[(0, *index)], sem.at[(1, *index)]

    pending = []

    barrier = pltpu.get_barrier_semaphore()
    for step in PLANE:
        pl.semaphore_signal(barrier, inc=1, device_id=plane_id(step), device_id_type=MESH_ID)
    for step in DEPTH:
        pl.semaphore_signal(barrier, inc=1, device_id=depth_id(step), device_id_type=MESH_ID)
    for device in (core_id, side_id):
        pl.semaphore_signal(barrier, inc=1, device_id=device, device_id_type=MESH_ID)

    tile_row = lax.broadcasted_iota(jnp.int32, (128, 128), 0)
    tile_col = lax.broadcasted_iota(jnp.int32, (128, 128), 1)
    norm_row = lax.broadcasted_iota(jnp.int32, (8, 128), 0)

    def right_gram(r, norms):
        piece = grad[:, pl.ds(pl.multiple_of(r * B, B), B)]
        part = lax.dot_general(piece, piece, (((0,), (0,)), ((), ())), preferred_element_type=F32)
        diag = jnp.zeros((128, 128), F32)
        for k in range(4):
            square = part[k * 128 : (k + 1) * 128, k * 128 : (k + 1) * 128]
            diag = diag + jnp.where(tile_row == tile_col, square, 0.0)
        lanes = jnp.sum(diag, axis=0, keepdims=True)
        gram[pl.ds(2 * r, 2)] = part.astype(BF16).reshape(2, 8, 32, B)
        return norms + jnp.where(norm_row == r, jnp.broadcast_to(lanes, (8, 128)), 0.0)

    norms = lax.fori_loop(0, 4, right_gram, jnp.zeros((8, 128), F32))
    norm_own[...] = norms
    lnorm[...] = norms
    xz[z] = prev_right[...]
    lroot[yl, c] = prev_left[0]

    pl.semaphore_wait(barrier, len(PLANE) + len(DEPTH) + 2)

    x_depth = [
        send(prev_right, xz.at[z], two(sem_xz, k), depth_id(step)) for k, step in enumerate(DEPTH)
    ]
    lx_core = send(prev_left.at[0], lroot.at[yl, c], two(sem_l, 0), core_id)
    lx_side = send(prev_left.at[0], lroot.at[yl, c], two(sem_l, 1), side_id)
    first = []
    for j, turn in enumerate((2, 1, 3, 0)):
        zz = ((z // 2 + turn) % 4) * 2
        rr = ((me_r + turn) % 4) * 2
        sent = []
        for k in range(7):
            a, b = plane_peer(PLANE[k])
            sent.append(
                send(
                    gram.at[a * 4 + b, pl.ds(zz, 2), :, pl.ds(0, CUT)], plane_in.at[k, j],
                    two(sem_plane, j, k), plane_id(PLANE[k]),
                )
            )
            sent.append(
                send(
                    gram.at[pl.ds(rr, 2), (z + DEPTH[k]) % 8, :, pl.ds(CUT, B - CUT)],
                    depth_in.at[k, j], two(sem_depth, j, k), depth_id(DEPTH[k]),
                )
            )
        first.append((zz, rr, sent))
        if j == 0:
            n_first = [
                send(norm_own, norm_p.at[k], two(sem_n1, k), plane_id(step))
                for k, step in enumerate(PLANE)
            ]
            n_core = send(lnorm, lnorm_in.at[0], two(sem_l, 2), core_id)

    def left_gram(i, carry):
        rows = grad[pl.ds(pl.multiple_of(i * 128, 128), 128), :]
        part = lax.dot_general(rows, grad[...], (((1,), (1,)), ((), ())), preferred_element_type=F32)
        lgram[i // 2, i % 2] = part.astype(BF16)
        return carry

    lax.fori_loop(0, 4, left_gram, 0)
    l_core = send(lgram.at[:, 1 - c], lin1, two(sem_l, 3), core_id)

    lx_side.wait_recv()
    lx_pass = send(lroot.at[1 - yl, c], lroot.at[1 - yl, c], two(sem_l, 4), core_id)
    n_core.wait()
    lnorm[...] = lnorm[...] + lnorm_in[0]
    n_side = send(lnorm, lnorm_in.at[1], two(sem_l, 5), side_id)

    for copy in x_depth:
        copy.wait_recv()
    xp[p] = xz[:, me_r]
    x_plane = []
    for k, step in enumerate(PLANE):
        a, b = plane_peer(step)
        x_plane.append(send(xz.at[:, (a * 4 + b) // 2], xp.at[p], two(sem_xp, k), plane_id(step)))

    l_core.wait_recv()
    lsum = lgram[:, c].astype(F32) + lin1[...].astype(F32)
    lsend[...] = lsum.astype(BF16)
    l_side = send(lsend.at[1 - yl], lin2, two(sem_l, 6), side_id)

    for copy in n_first:
        copy.wait_recv()
    total = norm_own[...]
    for k in range(7):
        total = total + norm_p[k]
    norm_mid[...] = total
    n_second = [
        send(norm_mid, norm_z.at[k], two(sem_n2, k), depth_id(step)) for k, step in enumerate(DEPTH)
    ]

    lx_core.wait_recv()
    lx_pass.wait_recv()
    n_side.wait()
    l_side.wait_recv()
    left_scale = jnp.sum(jnp.where(norm_row < 4, lnorm[...] + lnorm_in[1], 0.0)) / B + EPSILON
    left_rows = lsend[yl].astype(F32) + lin2[...].astype(F32)
    product = five_products(left_rows, lroot[...].reshape(B, B)) / left_scale
    left_new = (5.0 * prev_left[0].astype(F32) - product) / 4.0
    left_code = (left_new * pow_two(-exp_left[0])).astype(BF16)
    left_own[...] = left_code

    second = []
    for j in range(ROUNDS):
        zz, rr, sent = first[j]
        for copy in sent:
            copy.wait_recv()
        acc = gram[p, pl.ds(zz, 2), :, pl.ds(0, CUT)].astype(F32)
        for k in range(7):
            acc = acc + plane_in[k, j].astype(F32)
        plane_sum[j] = acc.astype(BF16)
        acc = gram[pl.ds(rr, 2), z, :, pl.ds(CUT, B - CUT)].astype(F32)
        for k in range(7):
            acc = acc + depth_in[k, j].astype(F32)
        depth_sum[j] = acc.astype(BF16)
        if j < ROUNDS - 1:
            for b in range(2):
                second.append(
                    send(plane_sum.at[j, b], strip_z.at[z], (sem_sz.at[0, 2 * j + b], sem_sz.at[1, z]),
                         (zz + b, yh, x, yl, c))
                )
                q = rr + b
                second.append(
                    send(depth_sum.at[j, b], strip_p.at[p], (sem_sp.at[0, 2 * j + b], sem_sp.at[1, p]),
                         (z, q // 4, q % 4, yl, c))
                )
        else:
            b = 1 - z % 2
            second.append(
                send(plane_sum.at[j, b], strip_z.at[z], (sem_sz.at[0, 6], sem_sz.at[1, z]),
                     (zz + b, yh, x, yl, c))
            )
            b = 1 - p % 2
            q = rr + b
            second.append(
                send(depth_sum.at[j, b], strip_p.at[p], (sem_sp.at[0, 6], sem_sp.at[1, p]),
                     (z, q // 4, q % 4, yl, c))
            )
    strip_z[z] = plane_sum[ROUNDS - 1, z % 2]
    strip_p[p] = depth_sum[ROUNDS - 1, p % 2]

    for copy in x_plane:
        copy.wait_recv()

    def lay(i, carry):
        rows = xp[:, i].astype(F32).reshape(64, B).astype(BF16)
        root[pl.ds(pl.multiple_of(i * 64, 64), 64), :] = rows
        return carry

    lax.fori_loop(0, 8, lay, 0)

    for copy in n_second:
        copy.wait_recv()
    total = norm_mid[...]
    for k in range(7):
        total = total + norm_z[k]
    right_scale = jnp.sum(jnp.where(norm_row == me_r, total, 0.0)) / B + EPSILON

    def arrived(buffer, sems, index):
        pltpu.make_async_remote_copy(
            src_ref=buffer.at[index], dst_ref=buffer.at[index], send_sem=sems.at[0, 0],
            recv_sem=sems.at[1, index], device_id=core_id, device_id_type=MESH_ID,
        ).wait_recv()

    for step in range(1, 8):
        arrived(strip_z, sem_sz, (z + step) % 8)
        arrived(strip_p, sem_sp, (p + step) % 8)
    acc_a = strip_z[0].astype(F32)
    acc_b = strip_p[0].astype(F32)
    for k in range(1, 8):
        acc_a = acc_a + strip_z[k].astype(F32)
        acc_b = acc_b + strip_p[k].astype(F32)
    rows = jnp.concatenate([acc_a, acc_b], axis=1)
    product = five_products(rows, root[...]) / right_scale
    start = root[pl.ds(pl.multiple_of((p % 2) * 256 + z * 32, 32), 32), :].astype(F32)
    right_new = (5.0 * start - product) / 4.0
    code[p, z] = (right_new * pow_two(-exp_right[me_r])).astype(BF16)

    to_depth = [
        send(code.at[p, z, :, pl.ds(0, CUT)], code.at[p, z, :, pl.ds(0, CUT)],
             two(sem_cz, k), depth_id(step))
        for k, step in enumerate(DEPTH)
    ]
    to_plane = [
        send(code.at[p, z], code.at[p, z], two(sem_cp, k), plane_id(step))
        for k, step in enumerate(PLANE)
    ]
    left_all[yl, c] = left_own[...]
    lc_core = send(left_own, lcode.at[yl, c], two(sem_l, 7), core_id)
    lc_side = send(left_own, lcode.at[yl, c], two(sem_l, 8), side_id)

    on_plane = []
    for i, dz in enumerate(DEPTH):
        to_depth[i].wait_recv()
        other = (z + 8 - dz) % 8
        for k, step in enumerate(PLANE):
            on_plane.append(
                send(code.at[p, other, :, pl.ds(0, CUT)], code.at[p, other, :, pl.ds(0, CUT)],
                     two(sem_fp, i, k), plane_id(step))
            )
    for copy in to_plane:
        copy.wait_recv()
    on_depth = [
        send(code.at[:, z, :, pl.ds(CUT, B - CUT)], code.at[:, z, :, pl.ds(CUT, B - CUT)],
             two(sem_fz, k), depth_id(step))
        for k, step in enumerate(DEPTH)
    ]
    lc_side.wait_recv()
    lc_pass = send(lcode.at[1 - yl, c], lcode.at[1 - yl, c], two(sem_l, 9), core_id)
    lc_core.wait_recv()
    lc_pass.wait_recv()
    left_all[yl, 1 - c] = lcode[yl, 1 - c]
    left_all[1 - yl] = lcode[1 - yl]
    for copy in on_plane:
        copy.wait_recv()
    for copy in on_depth:
        copy.wait_recv()

    owned = owner_of[z * 8 + p]
    for r in range(4):
        strip = code[2 * r + owned // 32, (owned // 4) % 8].astype(F32)
        picked = jnp.zeros((8, B), F32)
        for k in range(4):
            picked = picked + jnp.where(owned % 4 == k, strip[8 * k : 8 * k + 8], 0.0)
        right_own[r] = picked.astype(BF16)

    def mix(r, carry):
        columns = pl.ds(pl.multiple_of(r * B, B), B)
        full = code[pl.ds(2 * r, 2)].reshape(B, B)
        out = jnp.dot(grad[:, columns], full, preferred_element_type=F32)
        middle[:, columns] = (out * pow_two(exp_right[r])).astype(BF16)
        return carry

    lax.fori_loop(0, 4, mix, 0)

    for _, _, sent in first:
        for copy in sent:
            copy.wait_send()
    for copy in (
        x_depth + x_plane + n_first + n_second + second + to_depth + to_plane + on_plane + on_depth
        + [lx_core, lx_side, lx_pass, l_core, l_side, lc_core, lc_side, lc_pass]
    ):
        copy.wait_send()


def final_kernel(exp_left, left_all, middle, left_code, right_code, precond, root_left, root_right):
    out = jnp.dot(left_all[...], middle[...], preferred_element_type=F32)
    precond[...] = (out * pow_two(exp_left[0])).astype(BF16)
    root_left[0] = left_code[...]
    root_right[:, 0] = right_code[...]


def shards(grad, prev_left, prev_right, exp_left, exp_right, strip_owner):
    smem = pl.BlockSpec(memory_space=pltpu.SMEM)
    vmem = pl.BlockSpec(memory_space=pltpu.VMEM)
    dma = pltpu.SemaphoreType.DMA
    shape = jax.ShapeDtypeStruct
    middle, left_all, left_own, right_own = pl.pallas_call(
        exchange_kernel,
        out_shape=(
            shape((B, 4 * B), BF16), shape((2, 2, 128, B), BF16), shape((128, B), BF16),
            shape((4, 8, B), BF16),
        ),
        in_specs=[smem, smem, smem, vmem, vmem, vmem],
        out_specs=(vmem,) * 4,
        scratch_shapes=[
            pltpu.VMEM((8, 8, 32, B), BF16),
            pltpu.VMEM((7, ROUNDS, 2, 32, CUT), BF16),
            pltpu.VMEM((7, ROUNDS, 2, 32, B - CUT), BF16),
            pltpu.VMEM((ROUNDS, 2, 32, CUT), BF16),
            pltpu.VMEM((ROUNDS, 2, 32, B - CUT), BF16),
            pltpu.VMEM((8, 32, CUT), BF16),
            pltpu.VMEM((8, 32, B - CUT), BF16),
            pltpu.VMEM((8, 128), F32),
            pltpu.VMEM((8, 128), F32),
            pltpu.VMEM((7, 8, 128), F32),
            pltpu.VMEM((7, 8, 128), F32),
            pltpu.VMEM((8, 4, 8, B), BF16),
            pltpu.VMEM((8, 8, 8, B), BF16),
            pltpu.VMEM((B, B), BF16),
            pltpu.VMEM((8, 8, 32, B), BF16),
            pltpu.VMEM((2, 2, 128, B), BF16),
            pltpu.VMEM((2, 128, B), BF16),
            pltpu.VMEM((2, 128, B), BF16),
            pltpu.VMEM((128, B), BF16),
            pltpu.VMEM((2, 2, 128, B), BF16),
            pltpu.VMEM((2, 2, 128, B), BF16),
            pltpu.VMEM((8, 128), F32),
            pltpu.VMEM((2, 8, 128), F32),
            dma((2, ROUNDS, 7)), dma((2, ROUNDS, 7)), dma((2, 8)), dma((2, 8)),
            dma((2, 7)), dma((2, 7)), dma((2, 7)), dma((2, 7)),
            dma((2, 7)), dma((2, 7)), dma((2, 7, 7)), dma((2, 7)), dma((2, 10)),
        ],
        compiler_params=pltpu.CompilerParams(
            collective_id=0, has_side_effects=True, vmem_limit_bytes=40 << 20
        ),
        name="exchange",
    )(exp_left, exp_right, strip_owner, grad, prev_left, prev_right)
    return pl.pallas_call(
        final_kernel,
        grid=(4,),
        out_shape=(
            shape((B, 4 * B), BF16), shape((1, 128, B), BF16), shape((4, 1, 8, B), BF16),
        ),
        in_specs=[
            smem,
            pl.BlockSpec((B, B), lambda i: (0, 0)),
            pl.BlockSpec((B, B), lambda i: (0, i)),
            pl.BlockSpec((128, B), lambda i: (0, 0)),
            pl.BlockSpec((4, 8, B), lambda i: (0, 0, 0)),
        ],
        out_specs=(
            pl.BlockSpec((B, B), lambda i: (0, i)),
            pl.BlockSpec((1, 128, B), lambda i: (0, 0, 0)),
            pl.BlockSpec((4, 1, 8, B), lambda i: (0, 0, 0, 0)),
        ),
        name="final",
    )(exp_left, left_all.reshape(B, B), middle, left_own, right_own)


def solution(mesh):
    torus = Mesh(mesh.devices.reshape(8, 2, 4, 2, 2), AXES)
    in_specs = (
        P(GROUP, REPLICA),
        P(GROUP, REPLICA, None),
        P(REPLICA, GROUP, None),
        P(GROUP),
        P(REPLICA),
        P(),
    )
    out_specs = (P(GROUP, REPLICA), P(GROUP, REPLICA, None), P(REPLICA, GROUP, None, None))
    return jax.shard_map(
        shards, mesh=torus, in_specs=in_specs, out_specs=out_specs, check_vma=False
    )
```

```python
import contextlib

import jax
import jax.numpy as jnp
from jax import lax
from jax.experimental import pallas as pl
from jax.experimental.pallas import tpu as pltpu
from jax.sharding import Mesh
from jax.sharding import PartitionSpec as P

AXES = ("z", "yh", "x", "yl", "c")
GROUP = ("z", "yh", "x")
REPLICA = ("yl", "c")
MESH_ID = pl.DeviceIdType.MESH
F32 = jnp.float32
BF16 = jnp.bfloat16

EPSILON = 1e-06
B = 512
CUT = 384
ROUNDS = 4
PLANE = ((0, 1), (1, 0), (0, 3), (0, 2), (1, 1), (1, 3), (1, 2))
ROW = ((0, 1), (0, 3), (0, 2))
DEPTH = (1, 7, 2, 6, 3, 5, 4)


def pow_two(exponent):
    result = jnp.float32(0.0)
    for power in range(-4, 5):
        result = result + jnp.where(exponent == power, jnp.float32(2.0**power), jnp.float32(0.0))
    return result


def five_products(rows, root):
    count = rows.shape[0]
    for repeat in range(5):
        high = rows.astype(BF16)
        low = (rows - high.astype(F32)).astype(BF16)
        both = jnp.dot(jnp.concatenate([high, low], axis=0), root, preferred_element_type=F32)
        rows = both[:count] + both[count:]
    return rows


def exchange_kernel(
    exp_left_in, exp_right_in, owner_in, grad_in, prev_left_in, prev_right_in,
    middle_out, left_out, right_out,
    exp_left, exp_right, owner_of, grad, prev_left, prev_right,
    middle, left_own, right_own,
    gram_d, gram_o, plane_in, depth_in, plane_sum, depth_sum, strip_z, strip_p,
    turned, miss_a, miss_b,
    norm_own, norm_mid, norm_p, norm_z,
    xz, x_across, xp, root, code,
    lgram, lin1, lsend, lin2, lroot, lcode, lnorm, lnorm_in,
    sent, got, got_plane, got_depth, got_strip, got_pass, sem_l, sem_in,
):
    z, yh, x = lax.axis_index("z"), lax.axis_index("yh"), lax.axis_index("x")
    yl, c = lax.axis_index("yl"), lax.axis_index("c")
    p = yh * 4 + x
    across = (1 - yh) * 4 + x
    me_r = p // 2

    def plane_peer(step):
        return ((yh + step[0]) % 2, (x + step[1]) % 4)

    def plane_id(step):
        a, b = plane_peer(step)
        return (z, a, b, yl, c)

    def depth_id(step):
        return ((z + step) % 8, yh, x, yl, c)

    core_id = (z, yh, x, yl, 1 - c)
    side_id = (z, yh, x, 1 - yl, c)

    def send(src, dst, sems, device):
        copy = pltpu.make_async_remote_copy(
            src_ref=src, dst_ref=dst, send_sem=sems[0], recv_sem=sems[1],
            device_id=device, device_id_type=MESH_ID,
        )
        copy.start()
        return copy

    def two(sem, *index):
        return sem.at[(0, *index)], sem.at[(1, *index)]

    def all_sent(ref, sem):
        pltpu.make_async_remote_copy(
            src_ref=ref, dst_ref=ref, send_sem=sem, recv_sem=sem,
            device_id=core_id, device_id_type=MESH_ID,
        ).wait_send()

    def all_here(ref, sem):
        pltpu.make_async_remote_copy(
            src_ref=ref, dst_ref=ref, send_sem=sem, recv_sem=sem,
            device_id=core_id, device_id_type=MESH_ID,
        ).wait_recv()

    def fetch(src, dst, index):
        copy = pltpu.make_async_copy(src, dst, sem_in.at[index])
        copy.start()
        return copy

    get_right = fetch(prev_right_in, prev_right, 0)
    get_grad = [
        fetch(grad_in.at[:, pl.ds(r * B, B)], grad.at[:, pl.ds(r * B, B)], 1 + r) for r in range(4)
    ]
    get_rest = [
        fetch(prev_left_in, prev_left, 5), fetch(exp_left_in, exp_left, 6),
        fetch(exp_right_in, exp_right, 7), fetch(owner_in, owner_of, 8),
    ]

    barrier = pltpu.get_barrier_semaphore()
    for step in PLANE:
        pl.semaphore_signal(barrier, inc=1, device_id=plane_id(step), device_id_type=MESH_ID)
    for step in DEPTH:
        pl.semaphore_signal(barrier, inc=1, device_id=depth_id(step), device_id_type=MESH_ID)
    for device in (core_id, side_id):
        pl.semaphore_signal(barrier, inc=1, device_id=device, device_id_type=MESH_ID)

    tile_row = lax.broadcasted_iota(jnp.int32, (128, 128), 0)
    tile_col = lax.broadcasted_iota(jnp.int32, (128, 128), 1)
    norm_row = lax.broadcasted_iota(jnp.int32, (8, 128), 0)

    def right_gram(r, norms):
        pltpu.make_async_copy(
            grad_in.at[:, pl.ds(pl.multiple_of(r * B, B), B)],
            grad.at[:, pl.ds(pl.multiple_of(r * B, B), B)], sem_in.at[1 + r],
        ).wait()
        piece = grad[:, pl.ds(pl.multiple_of(r * B, B), B)]
        part = lax.dot_general(piece, piece, (((0,), (0,)), ((), ())), preferred_element_type=F32)
        diag = jnp.zeros((128, 128), F32)
        for k in range(4):
            tile = [
                part[k * 128 : (k + 1) * 128, n * 128 : (n + 1) * 128]
                for n in (k, (k + 1) % 4, (k + 2) % 4)
            ]
            diag = diag + jnp.where(tile_row == tile_col, tile[0], 0.0)
            side = jnp.concatenate(tile[1:], axis=1)
            gram_d[2 * r + k // 2, k % 2] = tile[0].reshape(8, 16, 128).astype(BF16)
            gram_o[2 * r + k // 2, k % 2] = side.reshape(8, 16, 256).astype(BF16)
        lanes = jnp.sum(diag, axis=0, keepdims=True)
        return norms + jnp.where(norm_row == r, jnp.broadcast_to(lanes, (8, 128)), 0.0)

    norms = lax.fori_loop(0, 4, right_gram, jnp.zeros((8, 128), F32))
    norm_own[...] = norms
    lnorm[...] = norms
    get_right.wait()
    for copy in get_rest:
        copy.wait()
    xz[z] = prev_right[...]
    lroot[yl, c] = prev_left[0]

    pl.semaphore_wait(barrier, len(PLANE) + len(DEPTH) + 2)

    for step in DEPTH:
        send(prev_right, xz.at[z], (sent.at[0], got.at[0]), depth_id(step))
    lx_core = send(prev_left.at[0], lroot.at[yl, c], two(sem_l, 0), core_id)
    lx_side = send(prev_left.at[0], lroot.at[yl, c], two(sem_l, 1), side_id)
    for k, step in enumerate(PLANE):
        send(norm_own, norm_p.at[k], (sent.at[3], got.at[1]), plane_id(step))
    n_core = send(lnorm, lnorm_in.at[0], two(sem_l, 2), core_id)
    first = []
    for j, turn in enumerate((2, 1, 3, 0)):
        zz = ((z // 2 + turn) % 4) * 2
        rr = ((me_r + turn) % 4) * 2
        first.append((zz, rr))
        for k in range(7):
            a, b = plane_peer(PLANE[k])
            send(
                gram_o.at[a * 4 + b, :, pl.ds(zz, 2)], plane_in.at[k, j],
                (sent.at[1], got_plane.at[j]), plane_id(PLANE[k]),
            )
            send(
                gram_d.at[pl.ds(rr, 2), :, (z + DEPTH[k]) % 8],
                depth_in.at[k, j], (sent.at[2], got_depth.at[j]), depth_id(DEPTH[k]),
            )

    def left_gram(i, carry):
        rows = grad[pl.ds(pl.multiple_of(i * 128, 128), 128), :]
        part = lax.dot_general(rows, grad[...], (((1,), (1,)), ((), ())), preferred_element_type=F32)
        lgram[i // 2, i % 2] = part.astype(BF16)
        return carry

    lax.fori_loop(0, 4, left_gram, 0)
    l_core = send(lgram.at[:, 1 - c], lin1, two(sem_l, 3), core_id)

    all_here(xz.at[pl.ds(0, 7)], got.at[0])
    x_pass = send(xz.at[:, pl.ds(2 - 2 * yh, 2)], x_across, two(sem_l, 10), plane_id((1, 0)))
    for step in ROW:
        b = (x + step[1]) % 4
        send(xz.at[:, 2 * yh + b // 2], xp.at[p], (sent.at[4], got.at[2]), plane_id(step))
    xp[p] = xz[:, me_r]

    l_core.wait_recv()
    lsum = lgram[:, c].astype(F32) + lin1[...].astype(F32)
    lsend[...] = lsum.astype(BF16)
    l_side = send(lsend.at[1 - yl], lin2, two(sem_l, 6), side_id)
    n_core.wait_recv()
    n_core.wait_send()
    lnorm[...] = lnorm[...] + lnorm_in[0]
    n_side = send(lnorm, lnorm_in.at[1], two(sem_l, 5), side_id)

    all_here(norm_p, got.at[1])
    total = norm_own[...]
    for k in range(7):
        total = total + norm_p[k]
    norm_mid[...] = total
    for k, step in enumerate(DEPTH):
        send(norm_mid, norm_z.at[k], (sent.at[5], got.at[3]), depth_id(step))

    x_pass.wait_recv()
    for step in ROW:
        b = (x + step[1]) % 4
        send(x_across.at[:, b // 2], xp.at[across], (sent.at[4], got.at[2]), plane_id(step))
    xp[across] = x_across[:, x // 2]

    lx_side.wait_recv()
    lx_pass = send(lroot.at[1 - yl, c], lroot.at[1 - yl, c], two(sem_l, 4), core_id)

    for j in range(ROUNDS):
        zz, rr = first[j]
        all_here(plane_in.at[:, j], got_plane.at[j])
        acc = gram_o[p, :, pl.ds(zz, 2)].astype(F32)
        for k in range(7):
            acc = acc + plane_in[k, j].astype(F32)
        plane_sum[:, pl.ds(zz, 2)] = acc.astype(BF16)
        all_here(depth_in.at[:, j], got_depth.at[j])
        acc = gram_d[pl.ds(rr, 2), :, z].astype(F32)
        for k in range(7):
            acc = acc + depth_in[k, j].astype(F32)
        depth_sum[j] = acc.astype(BF16)
        for b in range(2) if j < ROUNDS - 1 else (None,):
            bz = zz + (1 - z % 2 if b is None else b)
            send(plane_sum.at[:, bz], strip_z.at[z], (sent.at[6], got.at[4]), (bz, yh, x, yl, c))
            bp = 1 - p % 2 if b is None else b
            q = rr + bp
            send(depth_sum.at[j, bp], strip_p.at[p], (sent.at[7], got.at[5]),
                 (z, q // 4, q % 4, yl, c))
    strip_z[z] = plane_sum[:, z]
    strip_p[p] = depth_sum[ROUNDS - 1, p % 2]
    for b in range(2):
        block = plane_sum[b, :, :, pl.ds(0, 128)].astype(F32).reshape(128, 128)
        turned[b] = block.T.reshape(8, 16, 128).astype(BF16)
    mate = x + 1 - 2 * (x % 2)
    for step in DEPTH:
        there = (z + step) % 8
        send(turned.at[0, there], miss_b.at[z], (sent.at[12], got.at[9]), depth_id(step))
    for step in (0, *DEPTH):
        there = (z + step) % 8
        send(turned.at[1, there], miss_a.at[z], (sent.at[13], got.at[10]), (there, yh, mate, yl, c))
    miss_b[z] = turned[0, z]

    all_here(xp.at[pl.ds(0, 6)], got.at[2])

    def lay(i, carry):
        rows = xp[:, i].astype(F32).reshape(64, B).astype(BF16)
        root[pl.ds(pl.multiple_of(i * 64, 64), 64), :] = rows
        return carry

    lax.fori_loop(0, 8, lay, 0)

    all_here(norm_z, got.at[3])
    total = norm_mid[...]
    for k in range(7):
        total = total + norm_z[k]
    right_scale = jnp.sum(jnp.where(norm_row == me_r, total, 0.0)) / B + EPSILON

    lx_core.wait_recv()
    lx_pass.wait_recv()
    n_side.wait_recv()
    n_side.wait_send()
    l_side.wait_recv()
    left_scale = jnp.sum(jnp.where(norm_row < 4, lnorm[...] + lnorm_in[1], 0.0)) / B + EPSILON
    left_rows = lsend[yl].astype(F32) + lin2[...].astype(F32)
    product = five_products(left_rows, lroot[...].reshape(B, B)) / left_scale
    left_new = (5.0 * prev_left[0].astype(F32) - product) / 4.0
    left_code = (left_new * pow_two(-exp_left[0])).astype(BF16)
    left_own[...] = left_code

    all_here(strip_z.at[pl.ds(0, 7)], got.at[4])
    all_here(strip_p.at[pl.ds(0, 7)], got.at[5])
    all_here(miss_b.at[pl.ds(0, 7)], got.at[9])
    all_here(miss_a, got.at[10])

    def summed(ref):
        acc = ref[0].astype(F32)
        for k in range(1, 8):
            acc = acc + ref[k].astype(F32)
        return acc

    side, diag, low_a, low_b = summed(strip_z), summed(strip_p), summed(miss_a), summed(miss_b)
    even = p % 2 == 0
    one, two_on = side[:, :, :128], side[:, :, 128:]
    upper = jnp.where(
        even,
        jnp.concatenate([diag[0], one[0], two_on[0], low_a], axis=1),
        jnp.concatenate([two_on[0], low_a, diag[0], one[0]], axis=1),
    )
    lower = jnp.where(
        even,
        jnp.concatenate([low_b, diag[1], one[1], two_on[1]], axis=1),
        jnp.concatenate([one[1], two_on[1], low_b, diag[1]], axis=1),
    )
    rows = jnp.concatenate([upper, lower], axis=0)
    product = five_products(rows, root[...]) / right_scale
    offset = (p % 2) * 256 + z * 16
    start = jnp.concatenate(
        [root[pl.ds(pl.multiple_of(offset + b * 128, 16), 16), :] for b in range(2)], axis=0
    ).astype(F32)
    right_new = (5.0 * start - product) / 4.0
    right_code = (right_new * pow_two(-exp_right[me_r])).reshape(2, 16, B).astype(BF16)
    code[p, :, z] = right_code

    def near(q, layer):
        return code.at[q, :, layer, :, pl.ds(0, CUT)]

    for k, step in enumerate(DEPTH):
        send(near(p, z), near(p, z), (sent.at[8], got_strip.at[k]), depth_id(step))
    for step in PLANE:
        send(code.at[p, :, z], code.at[p, :, z], (sent.at[9], got.at[6]), plane_id(step))
    lcode[yl, c] = left_own[...]
    lc_core = send(left_own, lcode.at[yl, c], two(sem_l, 7), core_id)
    lc_side = send(left_own, lcode.at[yl, c], two(sem_l, 8), side_id)

    def pass_on(i):
        all_here(near(across, (z + 8 - DEPTH[i]) % 8), got_pass.at[i])
        for step in ROW:
            part = near(across, (z + 8 - DEPTH[i]) % 8)
            send(part, part, (sent.at[10], got.at[7]), plane_id(step))

    for i in range(7):
        part = near(p, (z + 8 - DEPTH[i]) % 8)
        all_here(part, got_strip.at[i])
        send(part, part, (sent.at[10], got_pass.at[i]), plane_id((1, 0)))
        for step in ROW:
            send(part, part, (sent.at[10], got.at[7]), plane_id(step))
        if i == 1:
            all_here(code.at[pl.ds(0, 7), :, 0], got.at[6])
            for step in DEPTH:
                part = code.at[:, :, z, :, pl.ds(CUT, B - CUT)]
                send(part, part, (sent.at[11], got.at[8]), depth_id(step))
        if i > 2:
            pass_on(i - 3)
    for i in range(4, 7):
        pass_on(i)
    lc_side.wait_recv()
    lc_pass = send(lcode.at[1 - yl, c], lcode.at[1 - yl, c], two(sem_l, 9), core_id)
    lc_core.wait_recv()
    lc_pass.wait_recv()
    puts = [pltpu.make_async_copy(lcode, left_out, sem_in.at[0])]
    puts[0].start()
    all_here(code.at[pl.ds(0, 6), :, pl.ds(0, 7), :, pl.ds(0, CUT)], got.at[7])
    all_here(code.at[:, :, pl.ds(0, 7), :, pl.ds(CUT, B - CUT)], got.at[8])

    owned = owner_of[z * 8 + p]
    for r in range(4):
        strip = code[2 * r + owned // 32, (owned // 16) % 2, (owned // 2) % 8].astype(F32)
        picked = jnp.where(owned % 2 == 0, strip[:8], strip[8:])
        right_own[r] = picked.astype(BF16)
    puts.append(pltpu.make_async_copy(right_own, right_out, sem_in.at[1]))
    puts[1].start()

    for r in range(4):
        columns = pl.ds(r * B, B)
        full = code[2 * r : 2 * r + 2].reshape(B, B)
        out = jnp.dot(grad[:, columns], full, preferred_element_type=F32)
        middle[:, columns] = (out * pow_two(exp_right[r])).astype(BF16)
        put = pltpu.make_async_copy(middle.at[:, columns], middle_out.at[:, columns], sem_in.at[2 + r])
        put.start()
        puts.append(put)
    for copy in puts:
        copy.wait()

    for k, ref in enumerate((
        xz.at[pl.ds(0, 7)], plane_in, depth_in, norm_p, xp.at[pl.ds(0, 6)], norm_z,
        strip_z.at[pl.ds(0, 7)], strip_p.at[pl.ds(0, 7)],
        code.at[0, :, pl.ds(0, 7), :, pl.ds(0, CUT)], code.at[0, :, pl.ds(0, 7)],
        code.at[pl.ds(0, 7), :, pl.ds(0, 7), :, pl.ds(0, CUT)],
        code.at[:, :, pl.ds(0, 7), :, pl.ds(CUT, B - CUT)],
        miss_b.at[pl.ds(0, 7)], miss_a,
    )):
        all_sent(ref, sent.at[k])
    for copy in (lx_core, lx_side, lx_pass, l_core, l_side, lc_core, lc_side, lc_pass, x_pass):
        copy.wait_send()


def final_kernel(
    exp_left_in, left_in, middle_in, right_in, precond, root_left, root_right,
    exp_left, left, middle, right, out, get_sem, put_sem,
):
    gets = [
        pltpu.make_async_copy(left_in, left, get_sem.at[0]),
        *[
            pltpu.make_async_copy(
                middle_in.at[:, pl.ds(r * B, B)], middle.at[:, pl.ds(r * B, B)], get_sem.at[1 + r]
            )
            for r in range(4)
        ],
        pltpu.make_async_copy(exp_left_in, exp_left, get_sem.at[5]),
        pltpu.make_async_copy(right_in, right, get_sem.at[6]),
    ]
    for get in gets:
        get.start()
    gets[0].wait()
    gets[5].wait()
    gets[6].wait()
    own = left.at[lax.axis_index("yl"), lax.axis_index("c")]
    puts = [
        pltpu.make_async_copy(own, root_left.at[0], put_sem.at[4]),
        pltpu.make_async_copy(right, root_right.at[:, 0], put_sem.at[5]),
    ]
    for put in puts:
        put.start()
    scale = pow_two(exp_left[0])
    for r in range(4):
        columns = pl.ds(r * B, B)
        gets[1 + r].wait()
        part = jnp.dot(left[...].reshape(B, B), middle[:, columns], preferred_element_type=F32)
        out[:, columns] = (part * scale).astype(BF16)
        put = pltpu.make_async_copy(out.at[:, columns], precond.at[:, columns], put_sem.at[r])
        put.start()
        puts.append(put)
    for put in puts:
        put.wait()


def shards(grad, prev_left, prev_right, exp_left, exp_right, strip_owner):
    anywhere = pl.BlockSpec(memory_space=pl.ANY)
    dma = pltpu.SemaphoreType.DMA
    shape = jax.ShapeDtypeStruct
    middle, left_all, right_own = pl.pallas_call(
        exchange_kernel,
        out_shape=(
            shape((B, 4 * B), BF16), shape((2, 2, 128, B), BF16), shape((4, 8, B), BF16),
        ),
        in_specs=[anywhere] * 6,
        out_specs=(anywhere,) * 3,
        scratch_shapes=[
            pltpu.SMEM((1,), jnp.int32), pltpu.SMEM((4,), jnp.int32), pltpu.SMEM((64,), jnp.int32),
            pltpu.VMEM((B, 4 * B), BF16),
            pltpu.VMEM((1, 128, B), BF16),
            pltpu.VMEM((4, 8, B), BF16),
            pltpu.VMEM((B, 4 * B), BF16),
            pltpu.VMEM((128, B), BF16),
            pltpu.VMEM((4, 8, B), BF16),
            pltpu.VMEM((8, 2, 8, 16, 128), BF16),
            pltpu.VMEM((8, 2, 8, 16, 256), BF16),
            pltpu.VMEM((7, ROUNDS, 2, 2, 16, 256), BF16),
            pltpu.VMEM((7, ROUNDS, 2, 2, 16, 128), BF16),
            pltpu.VMEM((2, 8, 16, 256), BF16),
            pltpu.VMEM((ROUNDS, 2, 2, 16, 128), BF16),
            pltpu.VMEM((8, 2, 16, 256), BF16),
            pltpu.VMEM((8, 2, 16, 128), BF16),
            pltpu.VMEM((2, 8, 16, 128), BF16),
            pltpu.VMEM((8, 16, 128), BF16),
            pltpu.VMEM((8, 16, 128), BF16),
            pltpu.VMEM((8, 128), F32),
            pltpu.VMEM((8, 128), F32),
            pltpu.VMEM((7, 8, 128), F32),
            pltpu.VMEM((7, 8, 128), F32),
            pltpu.VMEM((8, 4, 8, B), BF16),
            pltpu.VMEM((8, 2, 8, B), BF16),
            pltpu.VMEM((8, 8, 8, B), BF16),
            pltpu.VMEM((B, B), BF16),
            pltpu.VMEM((8, 2, 8, 16, B), BF16),
            pltpu.VMEM((2, 2, 128, B), BF16),
            pltpu.VMEM((2, 128, B), BF16),
            pltpu.VMEM((2, 128, B), BF16),
            pltpu.VMEM((128, B), BF16),
            pltpu.VMEM((2, 2, 128, B), BF16),
            pltpu.VMEM((2, 2, 128, B), BF16),
            pltpu.VMEM((8, 128), F32),
            pltpu.VMEM((2, 8, 128), F32),
            dma((14,)), dma((11,)), dma((ROUNDS,)), dma((ROUNDS,)), dma((7,)), dma((7,)),
            dma((2, 11)), dma((9,)),
        ],
        compiler_params=pltpu.CompilerParams(
            collective_id=0, has_side_effects=True, vmem_limit_bytes=54 << 20
        ),
        name="exchange",
    )(exp_left, exp_right, strip_owner, grad, prev_left, prev_right)
    return pl.pallas_call(
        final_kernel,
        out_shape=(
            shape((B, 4 * B), BF16), shape((1, 128, B), BF16), shape((4, 1, 8, B), BF16),
        ),
        in_specs=[anywhere] * 4,
        out_specs=(anywhere,) * 3,
        scratch_shapes=[
            pltpu.SMEM((1,), jnp.int32), pltpu.VMEM((2, 2, 128, B), BF16),
            pltpu.VMEM((B, 4 * B), BF16), pltpu.VMEM((4, 8, B), BF16),
            pltpu.VMEM((B, 4 * B), BF16), dma((7,)), dma((6,)),
        ],
        compiler_params=pltpu.CompilerParams(vmem_limit_bytes=54 << 20),
        name="final",
    )(exp_left, left_all, middle, right_own)


def solution(mesh):
    torus = Mesh(mesh.devices.reshape(8, 2, 4, 2, 2), AXES)
    in_specs = (
        P(GROUP, REPLICA),
        P(GROUP, REPLICA, None),
        P(REPLICA, GROUP, None),
        P(GROUP),
        P(REPLICA),
        P(),
    )
    out_specs = (P(GROUP, REPLICA), P(GROUP, REPLICA, None), P(REPLICA, GROUP, None, None))
    return jax.shard_map(
        shards, mesh=torus, in_specs=in_specs, out_specs=out_specs, check_vma=False
    )
```

```python
import contextlib

import jax
import jax.numpy as jnp
from jax import lax
from jax.experimental import pallas as pl
from jax.experimental.pallas import tpu as pltpu
from jax.sharding import Mesh
from jax.sharding import PartitionSpec as P

AXES = ("z", "yh", "x", "yl", "c")
GROUP = ("z", "yh", "x")
REPLICA = ("yl", "c")
MESH_ID = pl.DeviceIdType.MESH
F32 = jnp.float32
BF16 = jnp.bfloat16

EPSILON = 1e-06
B = 512
CUT = 384
ROUNDS = 4
PLANE = ((0, 1), (1, 0), (0, 3), (0, 2), (1, 1), (1, 3), (1, 2))
ROW = ((0, 1), (0, 3), (0, 2))
X_FIRST = (7, 0, 1)
DEPTH = (1, 7, 2, 6, 3, 5, 4)


def pow_two(exponent):
    result = jnp.float32(0.0)
    for power in range(-4, 5):
        result = result + jnp.where(exponent == power, jnp.float32(2.0**power), jnp.float32(0.0))
    return result


def five_products(rows, root):
    count = rows.shape[0]
    for repeat in range(5):
        high = rows.astype(BF16)
        low = (rows - high.astype(F32)).astype(BF16)
        both = jnp.dot(jnp.concatenate([high, low], axis=0), root, preferred_element_type=F32)
        rows = both[:count] + both[count:]
    return rows


def exchange_kernel(
    exp_left_in, exp_right_in, owner_in, grad_in, prev_left_in, prev_right_in,
    middle_out, left_out, right_out,
    exp_left, exp_right, owner_of, grad, prev_left, prev_right,
    middle, left_own, right_own,
    gram_d, gram_o, plane_in, depth_in, plane_sum, depth_sum, strip_z, strip_p,
    turned, miss_a, miss_b,
    norm_own, norm_mid, norm_p, norm_z,
    xz, x_across, xp, root, code,
    lgram, lin1, lsend, lin2, lroot, lcode, lnorm, lnorm_in,
    sent, got, got_plane, got_depth, got_strip, got_pass, got_row, sem_l, sem_in,
):
    z, yh, x = lax.axis_index("z"), lax.axis_index("yh"), lax.axis_index("x")
    yl, c = lax.axis_index("yl"), lax.axis_index("c")
    p = yh * 4 + x
    across = (1 - yh) * 4 + x
    me_r = p // 2

    def plane_peer(step):
        return ((yh + step[0]) % 2, (x + step[1]) % 4)

    def plane_id(step):
        a, b = plane_peer(step)
        return (z, a, b, yl, c)

    def depth_id(step):
        return ((z + step) % 8, yh, x, yl, c)

    core_id = (z, yh, x, yl, 1 - c)
    side_id = (z, yh, x, 1 - yl, c)

    def send(src, dst, sems, device):
        copy = pltpu.make_async_remote_copy(
            src_ref=src, dst_ref=dst, send_sem=sems[0], recv_sem=sems[1],
            device_id=device, device_id_type=MESH_ID,
        )
        copy.start()
        return copy

    def two(sem, *index):
        return sem.at[(0, *index)], sem.at[(1, *index)]

    def all_sent(ref, sem):
        pltpu.make_async_remote_copy(
            src_ref=ref, dst_ref=ref, send_sem=sem, recv_sem=sem,
            device_id=core_id, device_id_type=MESH_ID,
        ).wait_send()

    def all_here(ref, sem):
        pltpu.make_async_remote_copy(
            src_ref=ref, dst_ref=ref, send_sem=sem, recv_sem=sem,
            device_id=core_id, device_id_type=MESH_ID,
        ).wait_recv()

    def fetch(src, dst, index):
        copy = pltpu.make_async_copy(src, dst, sem_in.at[index])
        copy.start()
        return copy

    get_right = fetch(prev_right_in, prev_right, 0)
    get_grad = [
        fetch(grad_in.at[:, pl.ds(r * B, B)], grad.at[:, pl.ds(r * B, B)], 1 + r) for r in range(4)
    ]
    get_rest = [
        fetch(prev_left_in, prev_left, 5), fetch(exp_left_in, exp_left, 6),
        fetch(exp_right_in, exp_right, 7), fetch(owner_in, owner_of, 8),
    ]

    barrier = pltpu.get_barrier_semaphore()
    for step in PLANE:
        pl.semaphore_signal(barrier, inc=1, device_id=plane_id(step), device_id_type=MESH_ID)
    for step in DEPTH:
        pl.semaphore_signal(barrier, inc=1, device_id=depth_id(step), device_id_type=MESH_ID)
    for device in (core_id, side_id):
        pl.semaphore_signal(barrier, inc=1, device_id=device, device_id_type=MESH_ID)

    tile_row = lax.broadcasted_iota(jnp.int32, (128, 128), 0)
    tile_col = lax.broadcasted_iota(jnp.int32, (128, 128), 1)
    norm_row = lax.broadcasted_iota(jnp.int32, (8, 128), 0)

    def right_gram(r, norms):
        pltpu.make_async_copy(
            grad_in.at[:, pl.ds(pl.multiple_of(r * B, B), B)],
            grad.at[:, pl.ds(pl.multiple_of(r * B, B), B)], sem_in.at[1 + r],
        ).wait()
        piece = grad[:, pl.ds(pl.multiple_of(r * B, B), B)]
        part = lax.dot_general(piece, piece, (((0,), (0,)), ((), ())), preferred_element_type=F32)
        diag = jnp.zeros((128, 128), F32)
        for k in range(4):
            tile = [
                part[k * 128 : (k + 1) * 128, n * 128 : (n + 1) * 128]
                for n in (k, (k + 1) % 4, (k + 2) % 4)
            ]
            diag = diag + jnp.where(tile_row == tile_col, tile[0], 0.0)
            side = jnp.concatenate(tile[1:], axis=1)
            gram_d[2 * r + k // 2, k % 2] = tile[0].reshape(8, 16, 128).astype(BF16)
            gram_o[2 * r + k // 2, k % 2] = side.reshape(8, 16, 256).astype(BF16)
        lanes = jnp.sum(diag, axis=0, keepdims=True)
        return norms + jnp.where(norm_row == r, jnp.broadcast_to(lanes, (8, 128)), 0.0)

    norms = lax.fori_loop(0, 4, right_gram, jnp.zeros((8, 128), F32))
    norm_own[...] = norms
    lnorm[...] = norms
    get_right.wait()
    for copy in get_rest:
        copy.wait()
    xz[z] = prev_right[...]
    lroot[yl, c] = prev_left[0]

    pl.semaphore_wait(barrier, len(PLANE) + len(DEPTH) + 2)

    for step in DEPTH:
        send(prev_right, xz.at[z], (sent.at[0], got.at[0]), depth_id(step))
    lx_core = send(prev_left.at[0], lroot.at[yl, c], two(sem_l, 0), core_id)
    for k, step in enumerate(PLANE):
        send(norm_own, norm_p.at[k], (sent.at[3], got.at[1]), plane_id(step))
    n_core = send(lnorm, lnorm_in.at[0], two(sem_l, 2), core_id)
    first = [
        (((z // 2 + turn) % 4) * 2, ((me_r + turn) % 4) * 2) for turn in (2, 1, 3, 0)
    ]

    def plane_round(j):
        for k in range(7):
            a, b = plane_peer(PLANE[k])
            send(
                gram_o.at[a * 4 + b, :, pl.ds(first[j][0], 2)], plane_in.at[k, j],
                (sent.at[1], got_plane.at[j]), plane_id(PLANE[k]),
            )

    def depth_round(j):
        for k in range(7):
            send(
                gram_d.at[pl.ds(first[j][1], 2), :, (z + DEPTH[k]) % 8],
                depth_in.at[k, j], (sent.at[2], got_depth.at[j]), depth_id(DEPTH[k]),
            )

    for j in range(3):
        plane_round(j)

    def left_gram(i, carry):
        rows = grad[pl.ds(pl.multiple_of(i * 128, 128), 128), :]
        part = lax.dot_general(rows, grad[...], (((1,), (1,)), ((), ())), preferred_element_type=F32)
        lgram[i // 2, i % 2] = part.astype(BF16)
        return carry

    lax.fori_loop(0, 4, left_gram, 0)
    l_core = send(lgram.at[:, 1 - c], lin1, two(sem_l, 3), core_id)
    depth_round(0)

    all_here(xz.at[pl.ds(0, 7)], got.at[0])
    x_pass = send(xz.at[:, pl.ds(2 - 2 * yh, 2)], x_across, two(sem_l, 10), plane_id((1, 0)))
    plane_round(3)
    for step in ROW:
        b = (x + step[1]) % 4
        send(xz.at[:, 2 * yh + b // 2], xp.at[p], (sent.at[4], got.at[2]), plane_id(step))
    for j in range(1, ROUNDS):
        depth_round(j)
    xp[p] = xz[:, me_r]

    lx_side = send(prev_left.at[0], lroot.at[yl, c], two(sem_l, 1), side_id)
    l_core.wait_recv()
    lsum = lgram[:, c].astype(F32) + lin1[...].astype(F32)
    lsend[...] = lsum.astype(BF16)
    l_side = send(lsend.at[1 - yl], lin2, two(sem_l, 6), side_id)
    n_core.wait_recv()
    n_core.wait_send()
    lnorm[...] = lnorm[...] + lnorm_in[0]
    n_side = send(lnorm, lnorm_in.at[1], two(sem_l, 5), side_id)

    all_here(norm_p, got.at[1])
    total = norm_own[...]
    for k in range(7):
        total = total + norm_p[k]
    norm_mid[...] = total
    for k, step in enumerate(DEPTH):
        send(norm_mid, norm_z.at[k], (sent.at[5], got.at[3]), depth_id(step))

    x_pass.wait_recv()
    for step in ROW:
        b = (x + step[1]) % 4
        send(x_across.at[:, b // 2], xp.at[across], (sent.at[4], got.at[2]), plane_id(step))
    xp[across] = x_across[:, x // 2]

    for j in range(ROUNDS):
        zz, rr = first[j]
        all_here(plane_in.at[:, j], got_plane.at[j])
        acc = gram_o[p, :, pl.ds(zz, 2)].astype(F32)
        for k in range(7):
            acc = acc + plane_in[k, j].astype(F32)
        plane_sum[:, pl.ds(zz, 2)] = acc.astype(BF16)
        all_here(depth_in.at[:, j], got_depth.at[j])
        acc = gram_d[pl.ds(rr, 2), :, z].astype(F32)
        for k in range(7):
            acc = acc + depth_in[k, j].astype(F32)
        depth_sum[j] = acc.astype(BF16)
        for b in range(2) if j < ROUNDS - 1 else (None,):
            bz = zz + (1 - z % 2 if b is None else b)
            send(plane_sum.at[:, bz], strip_z.at[z], (sent.at[6], got.at[4]), (bz, yh, x, yl, c))
            bp = 1 - p % 2 if b is None else b
            q = rr + bp
            send(depth_sum.at[j, bp], strip_p.at[p], (sent.at[7], got.at[5]),
                 (z, q // 4, q % 4, yl, c))
    strip_z[z] = plane_sum[:, z]
    strip_p[p] = depth_sum[ROUNDS - 1, p % 2]
    for b in range(2):
        block = plane_sum[b, :, :, pl.ds(0, 128)].astype(F32).reshape(128, 128)
        turned[b] = block.T.reshape(8, 16, 128).astype(BF16)
    mate = x + 1 - 2 * (x % 2)
    for step in DEPTH:
        there = (z + step) % 8
        send(turned.at[0, there], miss_b.at[z], (sent.at[12], got.at[9]), depth_id(step))
    for step in (0, *DEPTH):
        there = (z + step) % 8
        send(turned.at[1, there], miss_a.at[z], (sent.at[13], got.at[10]), (there, yh, mate, yl, c))
    miss_b[z] = turned[0, z]

    lx_side.wait_recv()
    lx_pass = send(lroot.at[1 - yl, c], lroot.at[1 - yl, c], two(sem_l, 4), core_id)

    all_here(xp.at[pl.ds(0, 6)], got.at[2])

    def lay(i, carry):
        rows = xp[:, i].astype(F32).reshape(64, B).astype(BF16)
        root[pl.ds(pl.multiple_of(i * 64, 64), 64), :] = rows
        return carry

    lax.fori_loop(0, 8, lay, 0)

    all_here(norm_z, got.at[3])
    total = norm_mid[...]
    for k in range(7):
        total = total + norm_z[k]
    right_scale = jnp.sum(jnp.where(norm_row == me_r, total, 0.0)) / B + EPSILON

    all_here(strip_z.at[pl.ds(0, 7)], got.at[4])
    all_here(strip_p.at[pl.ds(0, 7)], got.at[5])
    all_here(miss_b.at[pl.ds(0, 7)], got.at[9])
    all_here(miss_a, got.at[10])

    def summed(ref):
        acc = ref[0].astype(F32)
        for k in range(1, 8):
            acc = acc + ref[k].astype(F32)
        return acc

    side, diag, low_a, low_b = summed(strip_z), summed(strip_p), summed(miss_a), summed(miss_b)
    even = p % 2 == 0
    one, two_on = side[:, :, :128], side[:, :, 128:]
    upper = jnp.where(
        even,
        jnp.concatenate([diag[0], one[0], two_on[0], low_a], axis=1),
        jnp.concatenate([two_on[0], low_a, diag[0], one[0]], axis=1),
    )
    lower = jnp.where(
        even,
        jnp.concatenate([low_b, diag[1], one[1], two_on[1]], axis=1),
        jnp.concatenate([one[1], two_on[1], low_b, diag[1]], axis=1),
    )
    rows = jnp.concatenate([upper, lower], axis=0)
    product = five_products(rows, root[...]) / right_scale
    offset = (p % 2) * 256 + z * 16
    start = jnp.concatenate(
        [root[pl.ds(pl.multiple_of(offset + b * 128, 16), 16), :] for b in range(2)], axis=0
    ).astype(F32)
    right_new = (5.0 * start - product) / 4.0
    right_code = (right_new * pow_two(-exp_right[me_r])).reshape(2, 16, B).astype(BF16)
    code[p, :, z] = right_code

    def near(q, layer):
        return code.at[q, :, layer, :, pl.ds(0, CUT)]

    for k, step in enumerate(DEPTH):
        send(near(p, z), near(p, z), (sent.at[8], got_strip.at[k]), depth_id(step))
    far = code.at[p, :, z, :, pl.ds(CUT, B - CUT)]
    for step in PLANE:
        send(far, far, (sent.at[9], got.at[6]), plane_id(step))
    layers = [(z + 8 - step) % 8 for step in DEPTH] + [z]

    def spread(i):
        part = near(p, layers[i])
        if i in X_FIRST:
            for step in ROW:
                send(part, part, (sent.at[10], got_row.at[X_FIRST.index(i)]), plane_id(step))
            return
        send(part, part, (sent.at[10], got_pass.at[i]), plane_id((1, 0)))
        for step in ROW:
            send(part, part, (sent.at[10], got.at[7]), plane_id(step))

    def cross(i):
        all_here(code.at[pl.ds(0, 3), :, 0, :, pl.ds(0, CUT)], got_row.at[X_FIRST.index(i)])
        for n in range(4):
            part = near(yh * 4 + n, layers[i])
            send(part, part, (sent.at[10], got.at[12]), plane_id((1, 0)))

    def pass_on(i):
        part = near(across, layers[i])
        all_here(part, got_pass.at[i])
        for step in ROW:
            send(part, part, (sent.at[10], got.at[11]), plane_id(step))

    spread(7)

    lx_core.wait_recv()
    lx_pass.wait_recv()
    n_side.wait_recv()
    n_side.wait_send()
    l_side.wait_recv()
    left_scale = jnp.sum(jnp.where(norm_row < 4, lnorm[...] + lnorm_in[1], 0.0)) / B + EPSILON
    left_rows = lsend[yl].astype(F32) + lin2[...].astype(F32)
    product = five_products(left_rows, lroot[...].reshape(B, B)) / left_scale
    left_new = (5.0 * prev_left[0].astype(F32) - product) / 4.0
    left_code = (left_new * pow_two(-exp_left[0])).astype(BF16)
    left_own[...] = left_code

    lcode[yl, c] = left_own[...]
    lc_core = send(left_own, lcode.at[yl, c], two(sem_l, 7), core_id)
    lc_side = send(left_own, lcode.at[yl, c], two(sem_l, 8), side_id)

    for i in range(7):
        all_here(near(p, layers[i]), got_strip.at[i])
        spread(i)
        if i == 1:
            all_here(code.at[pl.ds(0, 7), :, 0, :, pl.ds(CUT, B - CUT)], got.at[6])
            for step in DEPTH:
                part = code.at[:, :, z, :, pl.ds(CUT, B - CUT)]
                send(part, part, (sent.at[11], got.at[8]), depth_id(step))
            cross(7)
        if i in (3, 4):
            cross(i - 3)
        if i == 4:
            lc_side.wait_recv()
            lc_pass = send(lcode.at[1 - yl, c], lcode.at[1 - yl, c], two(sem_l, 9), core_id)
        if i > 4:
            pass_on(i - 3)
    for i in range(4, 7):
        pass_on(i)
    lc_core.wait_recv()
    lc_pass.wait_recv()
    puts = [pltpu.make_async_copy(lcode, left_out, sem_in.at[0])]
    puts[0].start()
    def mix(r, index, whole):
        columns = pl.ds(pl.multiple_of(r * B, B), B)
        full = code[pl.ds(2 * r, 2)].reshape(B, B)
        out = jnp.dot(grad[:, columns], full, preferred_element_type=F32)
        out = (out * pow_two(exp_right[r])).astype(BF16)
        if whole:
            out = jnp.dot(lcode[...].reshape(B, B), out, preferred_element_type=F32)
            out = (out * pow_two(exp_left[0])).astype(BF16)
        middle[:, columns] = out
        put = pltpu.make_async_copy(
            middle.at[:, columns], middle_out.at[:, columns], sem_in.at[2 + index]
        )
        put.start()
        puts.append(put)

    all_here(code.at[:, :, pl.ds(0, 7), :, pl.ds(CUT, B - CUT)], got.at[8])
    all_here(code.at[pl.ds(0, 3), :, pl.ds(0, 5), :, pl.ds(0, CUT)], got.at[7])
    for b in range(2):
        mix(2 * yh + b, b, True)
    all_here(code.at[pl.ds(0, 4), :, pl.ds(0, 3), :, pl.ds(0, CUT)], got.at[12])
    all_here(code.at[pl.ds(0, 3), :, pl.ds(0, 5), :, pl.ds(0, CUT)], got.at[11])
    for b in range(2):
        mix(2 - 2 * yh + b, 2 + b, False)

    owned = owner_of[z * 8 + p]
    for r in range(4):
        strip = code[2 * r + owned // 32, (owned // 16) % 2, (owned // 2) % 8].astype(F32)
        picked = jnp.where(owned % 2 == 0, strip[:8], strip[8:])
        right_own[r] = picked.astype(BF16)
    puts.append(pltpu.make_async_copy(right_own, right_out, sem_in.at[1]))
    puts[-1].start()
    for copy in puts:
        copy.wait()

    for k, ref in enumerate((
        xz.at[pl.ds(0, 7)], plane_in, depth_in, norm_p, xp.at[pl.ds(0, 6)], norm_z,
        strip_z.at[pl.ds(0, 7)], strip_p.at[pl.ds(0, 7)],
        code.at[0, :, pl.ds(0, 7), :, pl.ds(0, CUT)], code.at[0, :, pl.ds(0, 7), :, pl.ds(CUT, B - CUT)],
        code.at[pl.ds(0, 7), :, :, :, pl.ds(0, CUT)],
        code.at[:, :, pl.ds(0, 7), :, pl.ds(CUT, B - CUT)],
        miss_b.at[pl.ds(0, 7)], miss_a,
    )):
        all_sent(ref, sent.at[k])
    for copy in (lx_core, lx_side, lx_pass, l_core, l_side, lc_core, lc_side, lc_pass, x_pass):
        copy.wait_send()


def final_kernel(
    exp_left_in, left_in, middle_in, right_in, precond, root_left, root_right,
    exp_left, left, middle, right, out, get_sem, put_sem,
):
    yh = lax.axis_index("yh")
    blocks = [
        pl.ds(pl.multiple_of((2 - 2 * yh + r % 2 if r < 2 else 2 * yh + r % 2) * B, B), B)
        for r in range(4)
    ]
    gets = [
        pltpu.make_async_copy(left_in, left, get_sem.at[0]),
        *[
            pltpu.make_async_copy(middle_in.at[:, blocks[r]], middle.at[:, blocks[r]], get_sem.at[1 + r])
            for r in range(4)
        ],
        pltpu.make_async_copy(exp_left_in, exp_left, get_sem.at[5]),
        pltpu.make_async_copy(right_in, right, get_sem.at[6]),
    ]
    for get in gets:
        get.start()
    gets[0].wait()
    gets[5].wait()
    gets[6].wait()
    own = left.at[lax.axis_index("yl"), lax.axis_index("c")]
    puts = [
        pltpu.make_async_copy(own, root_left.at[0], put_sem.at[4]),
        pltpu.make_async_copy(right, root_right.at[:, 0], put_sem.at[5]),
    ]
    for put in puts:
        put.start()
    scale = pow_two(exp_left[0])
    for r in range(4):
        gets[1 + r].wait()
        if r < 2:
            part = jnp.dot(left[...].reshape(B, B), middle[:, blocks[r]], preferred_element_type=F32)
            out[:, blocks[r]] = (part * scale).astype(BF16)
        source = out if r < 2 else middle
        put = pltpu.make_async_copy(source.at[:, blocks[r]], precond.at[:, blocks[r]], put_sem.at[r])
        put.start()
        puts.append(put)
    for put in puts:
        put.wait()


def shards(grad, prev_left, prev_right, exp_left, exp_right, strip_owner):
    anywhere = pl.BlockSpec(memory_space=pl.ANY)
    dma = pltpu.SemaphoreType.DMA
    shape = jax.ShapeDtypeStruct
    middle, left_all, right_own = pl.pallas_call(
        exchange_kernel,
        out_shape=(
            shape((B, 4 * B), BF16), shape((2, 2, 128, B), BF16), shape((4, 8, B), BF16),
        ),
        in_specs=[anywhere] * 6,
        out_specs=(anywhere,) * 3,
        scratch_shapes=[
            pltpu.SMEM((1,), jnp.int32), pltpu.SMEM((4,), jnp.int32), pltpu.SMEM((64,), jnp.int32),
            pltpu.VMEM((B, 4 * B), BF16),
            pltpu.VMEM((1, 128, B), BF16),
            pltpu.VMEM((4, 8, B), BF16),
            pltpu.VMEM((B, 4 * B), BF16),
            pltpu.VMEM((128, B), BF16),
            pltpu.VMEM((4, 8, B), BF16),
            pltpu.VMEM((8, 2, 8, 16, 128), BF16),
            pltpu.VMEM((8, 2, 8, 16, 256), BF16),
            pltpu.VMEM((7, ROUNDS, 2, 2, 16, 256), BF16),
            pltpu.VMEM((7, ROUNDS, 2, 2, 16, 128), BF16),
            pltpu.VMEM((2, 8, 16, 256), BF16),
            pltpu.VMEM((ROUNDS, 2, 2, 16, 128), BF16),
            pltpu.VMEM((8, 2, 16, 256), BF16),
            pltpu.VMEM((8, 2, 16, 128), BF16),
            pltpu.VMEM((2, 8, 16, 128), BF16),
            pltpu.VMEM((8, 16, 128), BF16),
            pltpu.VMEM((8, 16, 128), BF16),
            pltpu.VMEM((8, 128), F32),
            pltpu.VMEM((8, 128), F32),
            pltpu.VMEM((7, 8, 128), F32),
            pltpu.VMEM((7, 8, 128), F32),
            pltpu.VMEM((8, 4, 8, B), BF16),
            pltpu.VMEM((8, 2, 8, B), BF16),
            pltpu.VMEM((8, 8, 8, B), BF16),
            pltpu.VMEM((B, B), BF16),
            pltpu.VMEM((8, 2, 8, 16, B), BF16),
            pltpu.VMEM((2, 2, 128, B), BF16),
            pltpu.VMEM((2, 128, B), BF16),
            pltpu.VMEM((2, 128, B), BF16),
            pltpu.VMEM((128, B), BF16),
            pltpu.VMEM((2, 2, 128, B), BF16),
            pltpu.VMEM((2, 2, 128, B), BF16),
            pltpu.VMEM((8, 128), F32),
            pltpu.VMEM((2, 8, 128), F32),
            dma((14,)), dma((13,)), dma((ROUNDS,)), dma((ROUNDS,)), dma((7,)), dma((7,)), dma((3,)),
            dma((2, 11)), dma((9,)),
        ],
        compiler_params=pltpu.CompilerParams(
            collective_id=0, has_side_effects=True, vmem_limit_bytes=54 << 20
        ),
        name="exchange",
    )(exp_left, exp_right, strip_owner, grad, prev_left, prev_right)
    return pl.pallas_call(
        final_kernel,
        out_shape=(
            shape((B, 4 * B), BF16), shape((1, 128, B), BF16), shape((4, 1, 8, B), BF16),
        ),
        in_specs=[anywhere] * 4,
        out_specs=(anywhere,) * 3,
        scratch_shapes=[
            pltpu.SMEM((1,), jnp.int32), pltpu.VMEM((2, 2, 128, B), BF16),
            pltpu.VMEM((B, 4 * B), BF16), pltpu.VMEM((4, 8, B), BF16),
            pltpu.VMEM((B, 4 * B), BF16), dma((7,)), dma((6,)),
        ],
        compiler_params=pltpu.CompilerParams(vmem_limit_bytes=54 << 20),
        name="final",
    )(exp_left, left_all, middle, right_own)


def solution(mesh):
    torus = Mesh(mesh.devices.reshape(8, 2, 4, 2, 2), AXES)
    in_specs = (
        P(GROUP, REPLICA),
        P(GROUP, REPLICA, None),
        P(REPLICA, GROUP, None),
        P(GROUP),
        P(REPLICA),
        P(),
    )
    out_specs = (P(GROUP, REPLICA), P(GROUP, REPLICA, None), P(REPLICA, GROUP, None, None))
    return jax.shard_map(
        shards, mesh=torus, in_specs=in_specs, out_specs=out_specs, check_vma=False
    )
```
